16 devices in a mesh: dpy: 2 (over z), dpx: 2 (over y), tp: 4 (over x, core).
Axes of the slice: x: 2, y: 2, z: 2, core: 2. Of those that a mesh axis runs over, the one named last changes fastest.
Arguments:
- x_saved: bfloat16 [2, 128, 512, 512], P(None, ('dpy', 'dpx'))
- y_saved: bfloat16 [2, 128, 512, 512], P(None, ('dpy', 'dpx'))
- d_out: bfloat16 [128, 512, 512], P(('dpy', 'dpx'))
- w_qkv: bfloat16 [2, 512, 3, 16, 32], P(None, None, None, 'tp')
- w_out: bfloat16 [2, 16, 32, 512], P(None, 'tp')
- w_up: bfloat16 [2, 512, 2048], P(None, None, 'tp')
- w_down: bfloat16 [2, 2048, 512], P(None, 'tp')
Outputs:
- output 1: bfloat16 [128, 512, 512], P(('dpy', 'dpx'))
- output 2: float32 [2, 512, 3, 16, 32], P(None, None, None, 'tp')
- output 3: float32 [2, 16, 32, 512], P(None, 'tp')
- output 4: float32 [2, 512, 2048], P(None, None, 'tp')
- output 5: float32 [2, 2048, 512], P(None, 'tp')
All inputs are finite; a program needn't handle non-finite values.
Results may differ from the reference program's by a relative error of at most 0.02.
Values are sent between devices in bfloat16 or wider.
A program may use at most 1 GiB of HBM per device.

```python
import jax
import jax.numpy as jnp
from jax import lax

WIDTH = 512
FFN = 2048
HEADS = 16
BATCH = 32
SEQ = 512
REPLICAS = 4
LAYERS = 2
HEAD_DIM = WIDTH // HEADS
SEQ_TOTAL = REPLICAS * BATCH


def setup_inputs(seed: int = 0) -> dict:
    root_key = jax.random.key(seed)
    sub_keys = jax.random.split(root_key, 7)
    act_shape = (LAYERS, SEQ_TOTAL, SEQ, WIDTH)
    x_saved = jax.random.normal(sub_keys[0], act_shape, jnp.float32).astype(jnp.bfloat16)
    y_saved = jax.random.normal(sub_keys[1], act_shape, jnp.float32).astype(jnp.bfloat16)
    d_out = jax.random.normal(sub_keys[2], (SEQ_TOTAL, SEQ, WIDTH), jnp.float32).astype(jnp.bfloat16)
    w_qkv = (jax.random.normal(sub_keys[3], (LAYERS, WIDTH, 3, HEADS, HEAD_DIM), jnp.float32) * WIDTH ** -0.5).astype(jnp.bfloat16)
    w_out = (jax.random.normal(sub_keys[4], (LAYERS, HEADS, HEAD_DIM, WIDTH), jnp.float32) * (4.0 * WIDTH ** -0.5)).astype(jnp.bfloat16)
    w_up = (jax.random.normal(sub_keys[5], (LAYERS, WIDTH, FFN), jnp.float32) * WIDTH ** -0.5).astype(jnp.bfloat16)
    w_down = (jax.random.normal(sub_keys[6], (LAYERS, FFN, WIDTH), jnp.float32) * (2.0 * FFN ** -0.5)).astype(jnp.bfloat16)
    return {'x_saved': x_saved, 'y_saved': y_saved, 'd_out': d_out, 'w_qkv': w_qkv, 'w_out': w_out, 'w_up': w_up, 'w_down': w_down}


def attention_backward(qkv_seq, d_att):
    queries = qkv_seq[:, 0].astype(jnp.float32)
    keys_all = qkv_seq[:, 1].astype(jnp.float32)
    values = qkv_seq[:, 2].astype(jnp.float32)
    datt_f32 = d_att.astype(jnp.float32)
    scale_factor = HEAD_DIM ** -0.5
    scores = jnp.einsum('qnd,knd->nqk', queries, keys_all) * scale_factor
    probs_f = jax.nn.softmax(scores, axis=-1)
    probs_b = probs_f.astype(jnp.bfloat16).astype(jnp.float32)
    att_out = jnp.einsum('nqk,knd->qnd', probs_b, values).astype(jnp.bfloat16)
    d_probs = jnp.einsum('qnd,knd->nqk', datt_f32, values)
    d_values = jnp.einsum('nqk,qnd->knd', probs_b, datt_f32).astype(jnp.bfloat16)
    row_dot = jnp.sum(d_probs * probs_f, axis=-1, keepdims=True)
    d_scores = (probs_f * (d_probs - row_dot) * scale_factor).astype(jnp.bfloat16).astype(jnp.float32)
    d_queries = jnp.einsum('nqk,knd->qnd', d_scores, keys_all).astype(jnp.bfloat16)
    d_keys = jnp.einsum('nqk,qnd->knd', d_scores, queries).astype(jnp.bfloat16)
    return att_out, jnp.stack([d_queries, d_keys, d_values], axis=1)


def layer_backward(x_in, y_mid, grad_out, wqkv_l, wout_l, wup_l, wdown_l):
    mid_f32 = y_mid.astype(jnp.float32)
    gout_f32 = grad_out.astype(jnp.float32)
    wup_f32 = wup_l.astype(jnp.float32)
    hidden = jnp.einsum('bsh,hf->bsf', mid_f32, wup_f32)
    act_f32, gelu_pull = jax.vjp(jax.nn.gelu, hidden)
    act_b = act_f32.astype(jnp.bfloat16).astype(jnp.float32)
    g_down = jnp.einsum('bsf,bsh->fh', act_b, gout_f32)
    d_act = jnp.einsum('bsh,fh->bsf', gout_f32, wdown_l.astype(jnp.float32))
    d_hidden = gelu_pull(d_act)[0].astype(jnp.bfloat16).astype(jnp.float32)
    g_up = jnp.einsum('bsh,bsf->hf', mid_f32, d_hidden)
    d_mid = (gout_f32 + jnp.einsum('bsf,hf->bsh', d_hidden, wup_f32)).astype(jnp.bfloat16)
    in_f32 = x_in.astype(jnp.float32)
    wqkv_f32 = wqkv_l.astype(jnp.float32)
    qkv = jnp.einsum('bsh,hcnd->bscnd', in_f32, wqkv_f32).astype(jnp.bfloat16)
    dmid_f32 = d_mid.astype(jnp.float32)
    d_att = jnp.einsum('bsh,ndh->bsnd', dmid_f32, wout_l.astype(jnp.float32)).astype(jnp.bfloat16)
    att_out, d_qkv = lax.map(lambda seq_pair: attention_backward(seq_pair[0], seq_pair[1]), (qkv, d_att))
    g_out = jnp.einsum('bsnd,bsh->ndh', att_out.astype(jnp.float32), dmid_f32)
    dqkv_f32 = d_qkv.astype(jnp.float32)
    g_qkv = jnp.einsum('bsh,bscnd->hcnd', in_f32, dqkv_f32)
    d_in = (dmid_f32 + jnp.einsum('bscnd,hcnd->bsh', dqkv_f32, wqkv_f32)).astype(jnp.bfloat16)
    return d_in, (g_qkv, g_out, g_up, g_down)


def reference(x_saved, y_saved, d_out, w_qkv, w_out, w_up, w_down):
    def replica_step(grad_sums, rep_idx):
        row_start = rep_idx * BATCH
        grad_cur = lax.dynamic_slice_in_dim(d_out, row_start, BATCH, axis=0)
        layer_grads = [None] * LAYERS
        for layer_idx in reversed(range(LAYERS)):
            x_in = lax.dynamic_slice_in_dim(x_saved[layer_idx], row_start, BATCH, axis=0)
            y_mid = lax.dynamic_slice_in_dim(y_saved[layer_idx], row_start, BATCH, axis=0)
            grad_cur, layer_grads[layer_idx] = layer_backward(x_in, y_mid, grad_cur, w_qkv[layer_idx], w_out[layer_idx], w_up[layer_idx], w_down[layer_idx])
        new_sums = tuple(sum_prev + jnp.stack([grad_set[slot_idx] for grad_set in layer_grads]) for slot_idx, sum_prev in enumerate(grad_sums))
        return new_sums, grad_cur

    init_sums = tuple(jnp.zeros(weight.shape, jnp.float32) for weight in (w_qkv, w_out, w_up, w_down))
    grad_sums, d_inputs = lax.scan(replica_step, init_sums, jnp.arange(REPLICAS))
    d_input = d_inputs.reshape(SEQ_TOTAL, SEQ, WIDTH)
    g_qkv, g_out, g_up, g_down = (sum_all / REPLICAS for sum_all in grad_sums)
    return d_input, g_qkv, g_out, g_up, g_down
```

```python
import functools

import jax
import jax.numpy as jnp
from jax import lax
from jax.experimental import pallas as pl
from jax.experimental.pallas import tpu as pltpu
from jax.sharding import PartitionSpec as P

F32 = jnp.float32
BF16 = jnp.bfloat16
LOG2E = 1.4426950408889634
GELU_C = 0.7978845608028654
GELU_K = 0.044715


def dot_nn(a, b):
    return lax.dot_general(a, b, (((1,), (0,)), ((), ())), preferred_element_type=F32)


def dot_nt(a, b):
    return lax.dot_general(a, b, (((1,), (1,)), ((), ())), preferred_element_type=F32)


def gelu_pair(h, da):
    h2 = h * h
    th = jnp.tanh(h * (GELU_C + (GELU_C * GELU_K) * h2))
    q = 0.5 + 0.5 * th
    act = h * q
    slope = (2.0 * GELU_C) + (6.0 * GELU_C * GELU_K) * h2
    dh = da * (q + act * ((1.0 - q) * slope))
    return act.astype(BF16), dh.astype(BF16)


def mlp_kernel(*refs):
    y_ref, g_ref = refs[0:2]
    up_refs, down_refs = refs[2:6], refs[6:10]
    gy_ref = refs[10]
    gup_refs, gdown_refs = refs[11:15], refs[15:19]
    upt_ref, yt_ref, dht_ref, acc_ref = refs[19:23]
    step = pl.program_id(0)

    @pl.when(step == 0)
    def _():
        for j in range(4):
            upt_ref[j] = up_refs[j][...].T
            gup_refs[j][...] = jnp.zeros_like(gup_refs[j])
            gdown_refs[j][...] = jnp.zeros_like(gdown_refs[j])

    y = y_ref[0]
    g = g_ref[0]
    yt_ref[...] = y.T
    blocks = [(j, k) for j in range(4) for k in range(2)]
    sub = 256

    def first(j, k):
        rows = slice(k * sub, (k + 1) * sub)
        return dot_nt(upt_ref[j, rows, :], y), dot_nt(down_refs[j][rows, :], g)

    held = first(*blocks[0])
    for i, (j, k) in enumerate(blocks):
        rows = slice(k * sub, (k + 1) * sub)
        nxt = first(*blocks[i + 1]) if i + 1 < len(blocks) else None
        at, dht = gelu_pair(*held)
        dht_ref[j, rows, :] = dht
        gdown_refs[j][rows, :] += dot_nn(at, g)
        gup_refs[j][:, rows] += dot_nt(yt_ref[...], dht)
        if k == 1:
            part = dot_nn(up_refs[j][...], dht_ref[j])
            if j == 0:
                acc_ref[...] = part
            else:
                acc_ref[...] += part
        held = nxt
    gy_ref[0] = (g.astype(F32) + acc_ref[...].T).astype(BF16)


def mlp_call(y, g, ups, downs):
    seqs, length, width = y.shape
    row = pl.BlockSpec((1, length, width), lambda s: (s, 0, 0))
    full = pl.BlockSpec((width, width), lambda s: (0, 0))
    grad = jax.ShapeDtypeStruct((width, width), F32)
    outs = pl.pallas_call(
        mlp_kernel,
        grid=(seqs,),
        in_specs=[row, row] + [full] * 8,
        out_specs=[row] + [full] * 8,
        out_shape=[jax.ShapeDtypeStruct(y.shape, BF16)] + [grad] * 8,
        scratch_shapes=[
            pltpu.VMEM((4, width, width), BF16),
            pltpu.VMEM((width, length), BF16),
            pltpu.VMEM((4, width, length), BF16),
            pltpu.VMEM((width, length), F32),
        ],
        compiler_params=pltpu.CompilerParams(
            dimension_semantics=("arbitrary",), vmem_limit_bytes=60 * 1024 * 1024
        ),
        cost_estimate=pl.CostEstimate(
            flops=10 * seqs * length * width * 4 * width, bytes_accessed=40 * 1024 * 1024, transcendentals=0
        ),
        name="mlp_bwd",
    )(y, g, *ups, *downs)
    return outs[0], outs[1:5], outs[5:9]


def att_kernel(heads, *refs):
    x_ref, gy_ref = refs[0:2]
    qkv_refs, out_refs = refs[2:6], refs[6:10]
    gx_ref = refs[10]
    gqkv_refs, gout_refs = refs[11:15], refs[15:19]
    wq_ref, wqt_ref, wo_ref, dqkv_ref, ot_ref, acc_ref, gq_ref, go_ref = refs[19:27]
    seq, grp = pl.program_id(0), pl.program_id(1)
    width = x_ref.shape[2]
    group = heads * 32

    @pl.when(jnp.logical_and(seq == 0, grp == 0))
    def _():
        for j in range(4):
            wq_ref[j] = qkv_refs[j][...]
            wqt_ref[j] = qkv_refs[j][...].T
            wo_ref[j] = out_refs[j][...]
        gq_ref[...] = jnp.zeros_like(gq_ref)
        go_ref[...] = jnp.zeros_like(go_ref)

    x = x_ref[0]
    gy = gy_ref[0]
    qkvt = dot_nt(wqt_ref[grp], x).astype(BF16)
    dot_ = dot_nt(wo_ref[grp], gy).astype(BF16)
    qt, kt, vt = qkvt[0:group], qkvt[group : 2 * group], qkvt[2 * group :]
    keys, values = kt.T, vt.T
    scale = 32 ** -0.5
    head_of = lax.broadcasted_iota(jnp.int32, qt.shape, 0) // 32

    def scores(n):
        own = head_of == n
        zero = jnp.zeros_like(qt)
        return dot_nn(keys, jnp.where(own, qt, zero)), dot_nn(values, jnp.where(own, dot_, zero))

    held = scores(0)
    for n in range(heads):
        rows = slice(32 * n, 32 * n + 32)
        nxt = scores(n + 1) if n + 1 < heads else None
        st, dpt = held
        top = jnp.max(st, axis=0, keepdims=True)
        e = jnp.exp2((st - top) * (scale * LOG2E))
        inv = 1.0 / jnp.sum(e, axis=0, keepdims=True)
        delta = jnp.sum(e * dpt, axis=0, keepdims=True) * inv
        pt = (e * inv).astype(BF16)
        dst = ((e * (inv * scale)) * (dpt - delta)).astype(BF16)
        ot_ref[rows] = dot_nn(vt[rows], pt).astype(BF16)
        dqkv_ref[2 * group + 32 * n : 2 * group + 32 * n + 32] = dot_nt(dot_[rows], pt).astype(BF16)
        dqkv_ref[rows] = dot_nn(kt[rows], dst).astype(BF16)
        dqkv_ref[group + 32 * n : group + 32 * n + 32] = dot_nt(qt[rows], dst).astype(BF16)
        held = nxt

    go_ref[grp] += dot_nn(ot_ref[...], gy)
    gq_ref[grp] += dot_nn(dqkv_ref[...], x)
    part = dot_nn(wq_ref[grp], dqkv_ref[...])

    @pl.when(grp == 0)
    def _():
        acc_ref[...] = part

    @pl.when(grp > 0)
    def _():
        acc_ref[...] += part

    @pl.when(grp == 3)
    def _():
        gx_ref[0] = (gy.astype(F32) + acc_ref[...].T).astype(BF16)

    @pl.when(jnp.logical_and(seq == pl.num_programs(0) - 1, grp == 3))
    def _():
        for j in range(4):
            gqkv_refs[j][...] = gq_ref[j].T
            gout_refs[j][...] = go_ref[j]


def att_call(x, gy, qkvs, outs_w):
    seqs, length, width = x.shape
    group = outs_w[0].shape[0]
    heads = group // 32
    row = pl.BlockSpec((1, length, width), lambda s, j: (s, 0, 0))
    wq = pl.BlockSpec((width, 3 * group), lambda s, j: (0, 0))
    wo = pl.BlockSpec((group, width), lambda s, j: (0, 0))
    outs = pl.pallas_call(
        functools.partial(att_kernel, heads),
        grid=(seqs, 4),
        in_specs=[row, row] + [wq] * 4 + [wo] * 4,
        out_specs=[row] + [wq] * 4 + [wo] * 4,
        out_shape=[jax.ShapeDtypeStruct(x.shape, BF16)]
        + [jax.ShapeDtypeStruct((width, 3 * group), F32)] * 4
        + [jax.ShapeDtypeStruct((group, width), F32)] * 4,
        scratch_shapes=[
            pltpu.VMEM((4, width, 3 * group), BF16),
            pltpu.VMEM((4, 3 * group, width), BF16),
            pltpu.VMEM((4, group, width), BF16),
            pltpu.VMEM((3 * group, length), BF16),
            pltpu.VMEM((group, length), BF16),
            pltpu.VMEM((width, length), F32),
            pltpu.VMEM((4, 3 * group, width), F32),
            pltpu.VMEM((4, group, width), F32),
        ],
        compiler_params=pltpu.CompilerParams(
            dimension_semantics=("arbitrary", "arbitrary"), vmem_limit_bytes=60 * 1024 * 1024
        ),
        cost_estimate=pl.CostEstimate(
            flops=60 * seqs * length * width * width, bytes_accessed=40 * 1024 * 1024, transcendentals=0
        ),
        name="att_bwd",
    )(x, gy, *qkvs, *outs_w)
    return outs[0], outs[1:5], outs[5:9]


def swap(a, bit):
    return lax.ppermute(a, "tp", [(i, i ^ bit) for i in range(4)])


def gather_rel(a):
    far = swap(a, 2)
    return [a, swap(a, 1), far, swap(far, 1)]


def reduce_rel(parts, data_axes):
    own = parts[0] + swap(parts[1], 1)
    far = parts[2] + swap(parts[3], 1)
    total = own + swap(far, 2)
    for axis in data_axes:
        total = total + lax.ppermute(total, axis, [(0, 1), (1, 0)])
    return total


def solution(mesh):
    data_axes = ("dpy", "dpx")
    replicas = mesh.shape["dpy"] * mesh.shape["dpx"]
    act_spec = P(None, data_axes, None, None)
    tok_spec = P(data_axes, None, None)
    qkv_spec = P(None, None, None, "tp", None)
    wout_spec = P(None, "tp", None, None)
    up_spec = P(None, None, "tp")
    down_spec = P(None, "tp", None)

    def device_backward(x_saved, y_saved, d_out, w_qkv, w_out, w_up, w_down):
        layers, width = w_qkv.shape[0], w_qkv.shape[1]
        heads, dim = w_qkv.shape[3:]
        mine = d_out.shape[0] // 4
        start = lax.axis_index("tp") * mine
        take = lambda a: lax.dynamic_slice_in_dim(a, start, mine, axis=0)
        grad = take(d_out)
        grads = [None] * layers
        for layer in reversed(range(layers)):
            ups, downs = gather_rel(w_up[layer]), gather_rel(w_down[layer])
            qkvs = gather_rel(w_qkv[layer].reshape(width, 3 * heads * dim))
            wouts = gather_rel(w_out[layer].reshape(heads * dim, width))
            mid, gup, gdown = mlp_call(take(y_saved[layer]), grad, ups, downs)
            grad, gqkv, gout = att_call(take(x_saved[layer]), mid, qkvs, wouts)
            sums = [reduce_rel(parts, data_axes) / replicas for parts in (gqkv, gout, gup, gdown)]
            grads[layer] = (
                sums[0].reshape(width, 3, heads, dim),
                sums[1].reshape(heads, dim, width),
                sums[2],
                sums[3],
            )
        d_input = lax.all_gather(grad, "tp", axis=0, tiled=True)
        return (d_input,) + tuple(jnp.stack([g[slot] for g in grads]) for slot in range(4))

    return jax.shard_map(
        device_backward,
        mesh=mesh,
        in_specs=(act_spec, act_spec, tok_spec, qkv_spec, wout_spec, up_spec, down_spec),
        out_specs=(tok_spec, qkv_spec, wout_spec, up_spec, down_spec),
        check_vma=False,
    )
```

```python
import functools

import jax
import jax.numpy as jnp
from jax import lax
from jax.experimental import pallas as pl
from jax.experimental.pallas import tpu as pltpu
from jax.sharding import PartitionSpec as P

F32 = jnp.float32
BF16 = jnp.bfloat16
MESH = pl.DeviceIdType.MESH
LOG2E = 1.4426950408889634
GELU_C = 0.7978845608028654
GELU_K = 0.044715
TP = 4
DIM = 32
VMEM_LIMIT = 60 * 1024 * 1024


def dot_nn(a, b):
    return lax.dot_general(a, b, (((1,), (0,)), ((), ())), preferred_element_type=F32)


def dot_nt(a, b):
    return lax.dot_general(a, b, (((1,), (1,)), ((), ())), preferred_element_type=F32)


def first_row(seqs):
    return lax.axis_index("tp") * seqs


def gelu_pair(h, da):
    h2 = h * h
    th = jnp.tanh(h * (GELU_C + (GELU_C * GELU_K) * h2))
    q = 0.5 + 0.5 * th
    act = h * q
    slope = (2.0 * GELU_C) + (6.0 * GELU_C * GELU_K) * h2
    dh = da * (q + act * ((1.0 - q) * slope))
    return act.astype(BF16), dh.astype(BF16)


def mlp_kernel(y_ref, g_ref, w_ref, gy_ref, gw_ref, upt_ref, yt_ref, dht_ref, acc_ref):
    step = pl.program_id(0)
    width = y_ref.shape[-1]

    @pl.when(step == 0)
    def _():
        for j in range(TP):
            upt_ref[j] = w_ref[j, 0:width].T
        gw_ref[...] = jnp.zeros_like(gw_ref)

    y = y_ref[...]
    g = g_ref[...]
    yt_ref[...] = y.T
    sub = 256
    blocks = [(j, k) for j in range(TP) for k in range(width // sub)]

    def first(j, k):
        rows = slice(k * sub, (k + 1) * sub)
        return dot_nt(upt_ref[j, rows, :], y), dot_nt(w_ref[j, width + k * sub : width + (k + 1) * sub], g)

    held = first(*blocks[0])
    for i, (j, k) in enumerate(blocks):
        rows = slice(k * sub, (k + 1) * sub)
        nxt = first(*blocks[i + 1]) if i + 1 < len(blocks) else None
        at, dht = gelu_pair(*held)
        dht_ref[j, rows, :] = dht
        gw_ref[j, width + k * sub : width + (k + 1) * sub] += dot_nn(at, g)
        gw_ref[j, 0:width, rows] += dot_nt(yt_ref[...], dht)
        if k == 1:
            part = dot_nn(w_ref[j, 0:width], dht_ref[j])
            if j == 0:
                acc_ref[...] = part
            else:
                acc_ref[...] += part
        held = nxt
    gy_ref[...] = (g.astype(F32) + acc_ref[...].T).astype(BF16)


def mlp_call(y_saved, layer, g, g_is_part, w):
    length, width = y_saved.shape[2:]
    seqs = y_saved.shape[1] // TP
    g_map = (lambda s: (s, 0, 0)) if g_is_part else (lambda s: (first_row(seqs) + s, 0, 0))
    return pl.pallas_call(
        mlp_kernel,
        grid_spec=pltpu.PrefetchScalarGridSpec(
            num_scalar_prefetch=0,
            grid=(seqs,),
            in_specs=[
                pl.BlockSpec((None, None, length, width), lambda s: (layer, first_row(seqs) + s, 0, 0)),
                pl.BlockSpec((None, length, width), g_map),
                pl.BlockSpec(w.shape, lambda s: (0, 0, 0)),
            ],
            out_specs=[
                pl.BlockSpec((None, length, width), lambda s: (s, 0, 0)),
                pl.BlockSpec(w.shape, lambda s: (0, 0, 0)),
            ],
            scratch_shapes=[
                pltpu.VMEM((TP, width, width), BF16),
                pltpu.VMEM((width, length), BF16),
                pltpu.VMEM((TP, width, length), BF16),
                pltpu.VMEM((width, length), F32),
            ],
        ),
        out_shape=[jax.ShapeDtypeStruct((seqs, length, width), BF16), jax.ShapeDtypeStruct(w.shape, F32)],
        compiler_params=pltpu.CompilerParams(dimension_semantics=("arbitrary",), vmem_limit_bytes=VMEM_LIMIT),
        cost_estimate=pl.CostEstimate(
            flops=10 * seqs * length * width * 4 * width, bytes_accessed=40 * 1024 * 1024, transcendentals=0
        ),
        name="mlp_bwd",
    )(y_saved, g, w)


def att_math(grp, x, gy, w_ref, wq_ref, gw_ref, dqkv_ref, ot_ref, acc_ref):
    group = wq_ref.shape[2] // 3
    heads = group // DIM
    qkvt = dot_nt(w_ref[grp, 0 : 3 * group], x).astype(BF16)
    dot_ = dot_nt(w_ref[grp, 3 * group :], gy).astype(BF16)
    qt, kt, vt = qkvt[0:group], qkvt[group : 2 * group], qkvt[2 * group :]
    keys, values = kt.T, vt.T
    scale = DIM ** -0.5
    head_of = lax.broadcasted_iota(jnp.int32, qt.shape, 0) // DIM

    def scores(n):
        own = head_of == n
        zero = jnp.zeros_like(qt)
        return dot_nn(keys, jnp.where(own, qt, zero)), dot_nn(values, jnp.where(own, dot_, zero))

    held = scores(0)
    for n in range(heads):
        rows = slice(DIM * n, DIM * (n + 1))
        nxt = scores(n + 1) if n + 1 < heads else None
        st, dpt = held
        top = jnp.max(st, axis=0, keepdims=True)
        e = jnp.exp2((st - top) * (scale * LOG2E))
        inv = 1.0 / jnp.sum(e, axis=0, keepdims=True)
        delta = jnp.sum(e * dpt, axis=0, keepdims=True) * inv
        pt = (e * inv).astype(BF16)
        dst = ((e * (inv * scale)) * (dpt - delta)).astype(BF16)
        ot_ref[rows] = dot_nn(vt[rows], pt).astype(BF16)
        dqkv_ref[2 * group + DIM * n : 2 * group + DIM * (n + 1)] = dot_nt(dot_[rows], pt).astype(BF16)
        dqkv_ref[rows] = dot_nn(kt[rows], dst).astype(BF16)
        dqkv_ref[group + DIM * n : group + DIM * (n + 1)] = dot_nt(qt[rows], dst).astype(BF16)
        held = nxt

    gw_ref[grp, 3 * group :] += dot_nn(ot_ref[...], gy)
    gw_ref[grp, 0 : 3 * group] += dot_nn(dqkv_ref[...], x)
    part = dot_nn(wq_ref[grp], dqkv_ref[...])

    @pl.when(grp == 0)
    def _():
        acc_ref[...] = part

    @pl.when(grp > 0)
    def _():
        acc_ref[...] += part


def att_setup(w_ref, wq_ref, gw_ref):
    for j in range(TP):
        wq_ref[j] = w_ref[j, 0 : wq_ref.shape[2]].T
    gw_ref[...] = jnp.zeros_like(gw_ref)


def att_kernel(x_ref, gy_ref, w_ref, gx_ref, gw_ref, wq_ref, dqkv_ref, ot_ref, acc_ref):
    seq, grp = pl.program_id(0), pl.program_id(1)

    @pl.when(jnp.logical_and(seq == 0, grp == 0))
    def _():
        att_setup(w_ref, wq_ref, gw_ref)

    gy = gy_ref[...]
    att_math(grp, x_ref[...], gy, w_ref, wq_ref, gw_ref, dqkv_ref, ot_ref, acc_ref)

    @pl.when(grp == TP - 1)
    def _():
        gx_ref[...] = (gy.astype(F32) + acc_ref[...].T).astype(BF16)


def att_share_kernel(
    x_ref, gy_ref, w_ref, full_ref, gw_ref,
    wq_ref, dqkv_ref, ot_ref, acc_ref, gxb_ref, own_sem, send_sem, recv_sem,
):
    seq, grp = pl.program_id(0), pl.program_id(1)
    seqs = pl.num_programs(0)
    me = lax.axis_index("tp")
    near = me + 1 - 2 * (me % 2)
    far = (me + 2) % TP

    def keep(s):
        return pltpu.make_async_copy(gxb_ref.at[s % 2], full_ref.at[me * seqs + s], own_sem.at[s % 2])

    def send(kind, s):
        row = (far if kind == 2 else me) * seqs + s
        return pltpu.make_async_remote_copy(
            full_ref.at[row], full_ref.at[row], send_sem.at[kind, s], recv_sem.at[kind, s],
            device_id={"tp": far if kind == 1 else near}, device_id_type=MESH,
        )

    def arrived(kind, s):
        owner = (near, far, (near + 2) % TP)[kind]
        row = owner * seqs + s
        return pltpu.make_async_remote_copy(
            full_ref.at[row], full_ref.at[row], send_sem.at[kind, s], recv_sem.at[kind, s],
            device_id={"tp": far if kind == 1 else near}, device_id_type=MESH,
        )

    @pl.when(jnp.logical_and(seq == 0, grp == 0))
    def _():
        barrier = pltpu.get_barrier_semaphore()
        for peer in (near, far):
            pl.semaphore_signal(barrier, inc=1, device_id={"tp": peer}, device_id_type=MESH)
        pl.semaphore_wait(barrier, 2)
        att_setup(w_ref, wq_ref, gw_ref)

    @pl.when(jnp.logical_and(seq > 0, grp == 0))
    def _():
        keep(seq - 1).wait()
        send(0, seq - 1).start()
        send(1, seq - 1).start()

    @pl.when(jnp.logical_and(seq > 0, grp == 2))
    def _():
        arrived(1, seq - 1).wait_recv()
        send(2, seq - 1).start()

    gy = gy_ref[...]
    att_math(grp, x_ref[...], gy, w_ref, wq_ref, gw_ref, dqkv_ref, ot_ref, acc_ref)

    @pl.when(grp == TP - 1)
    def _():
        gxb_ref[seq % 2] = (gy.astype(F32) + acc_ref[...].T).astype(BF16)
        keep(seq).start()

    @pl.when(jnp.logical_and(seq == seqs - 1, grp == TP - 1))
    def _():
        keep(seq).wait()
        send(0, seq).start()
        send(1, seq).start()
        arrived(1, seq).wait_recv()
        send(2, seq).start()

        @pl.loop(0, seqs)
        def _(s):
            for kind in range(3):
                send(kind, s).wait_send()
            arrived(0, s).wait_recv()
            arrived(2, s).wait_recv()


def att_call(x_saved, layer, gy, w, share):
    length, width = x_saved.shape[2:]
    seqs = x_saved.shape[1] // TP
    group = w.shape[1] // 4
    scratch = [
        pltpu.VMEM((TP, width, 3 * group), BF16),
        pltpu.VMEM((3 * group, length), BF16),
        pltpu.VMEM((group, length), BF16),
        pltpu.VMEM((width, length), F32),
    ]
    row = pl.BlockSpec((None, length, width), lambda s, j: (s, 0, 0))
    whole = pl.BlockSpec(w.shape, lambda s, j: (0, 0, 0))
    if share:
        scratch += [
            pltpu.VMEM((2, length, width), BF16),
            pltpu.SemaphoreType.DMA((2,)),
            pltpu.SemaphoreType.DMA((3, seqs)),
            pltpu.SemaphoreType.DMA((3, seqs)),
        ]
        gx_shape = jax.ShapeDtypeStruct(x_saved.shape[1:], BF16)
        gx_spec = pl.BlockSpec(memory_space=pl.ANY)
    else:
        gx_shape = jax.ShapeDtypeStruct((seqs, length, width), BF16)
        gx_spec = row
    return pl.pallas_call(
        att_share_kernel if share else att_kernel,
        grid_spec=pltpu.PrefetchScalarGridSpec(
            num_scalar_prefetch=0,
            grid=(seqs, TP),
            in_specs=[
                pl.BlockSpec((None, None, length, width), lambda s, j: (layer, first_row(seqs) + s, 0, 0)),
                row,
                whole,
            ],
            out_specs=[gx_spec, whole],
            scratch_shapes=scratch,
        ),
        out_shape=[gx_shape, jax.ShapeDtypeStruct(w.shape, F32)],
        compiler_params=pltpu.CompilerParams(
            dimension_semantics=("arbitrary", "arbitrary"),
            vmem_limit_bytes=VMEM_LIMIT,
            **({"collective_id": 0, "has_side_effects": True} if share else {}),
        ),
        cost_estimate=pl.CostEstimate(
            flops=60 * seqs * length * width * width, bytes_accessed=40 * 1024 * 1024, transcendentals=0
        ),
        name="att_bwd_share" if share else "att_bwd",
    )(x_saved, gy, w)


def solution(mesh):
    data_axes = ("dpy", "dpx")
    replicas = mesh.shape["dpy"] * mesh.shape["dpx"]
    act_spec = P(None, data_axes, None, None)
    tok_spec = P(data_axes, None, None)
    qkv_spec = P(None, None, None, "tp", None)
    wout_spec = P(None, "tp", None, None)
    up_spec = P(None, None, "tp")
    down_spec = P(None, "tp", None)

    def device_backward(x_saved, y_saved, d_out, w_qkv, w_out, w_up, w_down):
        layers, width, _, heads, dim = w_qkv.shape
        group = heads * dim
        w_qkvt = w_qkv.transpose(0, 2, 3, 4, 1).reshape(layers, 3 * group, width)
        gather = lambda *parts: lax.all_gather(jnp.concatenate(parts, axis=0), "tp", axis=0, tiled=False)
        mlp_w, att_w = [None] * layers, [None] * layers
        for layer in reversed(range(layers)):
            mlp_w[layer] = gather(w_up[layer], w_down[layer])
            att_w[layer] = gather(w_qkvt[layer], w_out[layer].reshape(group, width))

        def total(parts):
            mine = lax.psum_scatter(parts, "tp", scatter_dimension=0, tiled=False)
            return lax.psum(mine, data_axes) / replicas

        mlp_g, att_g = [None] * layers, [None] * layers
        grad = d_out
        for layer in reversed(range(layers)):
            mid, mlp_g[layer] = mlp_call(y_saved, layer, grad, layer < layers - 1, mlp_w[layer])
            grad, att_g[layer] = att_call(x_saved, layer, mid, att_w[layer], layer == 0)
        mlp_g, att_g = [total(g) for g in mlp_g], [total(g) for g in att_g]
        g_qkvt = jnp.stack([g[: 3 * group] for g in att_g]).reshape(layers, 3, heads, dim, width)
        return (
            grad,
            g_qkvt.transpose(0, 4, 1, 2, 3),
            jnp.stack([g[3 * group :] for g in att_g]).reshape(layers, heads, dim, width),
            jnp.stack([g[:width] for g in mlp_g]),
            jnp.stack([g[width:] for g in mlp_g]),
        )

    return jax.shard_map(
        device_backward,
        mesh=mesh,
        in_specs=(act_spec, act_spec, tok_spec, qkv_spec, wout_spec, up_spec, down_spec),
        out_specs=(tok_spec, qkv_spec, wout_spec, up_spec, down_spec),
        check_vma=False,
    )
```
